32 devices in a mesh: dp: 16 (over z, x, core), tp: 2 (over y).
Axes of the slice: x: 2, y: 2, z: 4, core: 2. Of those that a mesh axis runs over, the one named last changes fastest.
Arguments:
- tokens: bfloat16 [4096, 2048], P(('dp', 'tp')), may hold values from -6 to 6
- gain_attn: bfloat16 [2048], P('dp'), may hold values from 0.5 to 1.5
- query_weight: bfloat16 [2048, 2048], P('dp', 'tp'), may hold values from -0.125 to 0.125
- key_matrix: bfloat16 [2048, 512], P('dp', 'tp'), may hold values from -0.125 to 0.125
- value_matrix: bfloat16 [2048, 512], P('dp', 'tp'), may hold values from -0.125 to 0.125
- out_weight: bfloat16 [2048, 2048], P('tp', 'dp'), may hold values from -1 to 1
- gain_ffn: bfloat16 [2048], P('dp'), may hold values from 0.5 to 1.5
- gate_weight: bfloat16 [2048, 8192], P('dp', 'tp'), may hold values from -0.125 to 0.125
- up_weight: bfloat16 [2048, 8192], P('dp', 'tp'), may hold values from -0.125 to 0.125
- down_weight: bfloat16 [8192, 2048], P('tp', 'dp'), may hold values from -0.0625 to 0.0625
- cotangent: bfloat16 [4096, 2048], P(('dp', 'tp')), may hold values from -6 to 6
- seq_lens: int32 [16], P('dp'), may hold values from 128 to 256, as said below
- pad_mask: int32 [4096], P('dp'), may hold values from 0 to 1, as said below
- positions: int32 [4096], P('dp'), may hold values from 0 to 255, as said below
Outputs:
- output: bfloat16 [4096, 2048], P(('dp', 'tp'))
- grad_tokens: float32 [4096, 2048], P(('dp', 'tp'))
- grad_gain_attn: float32 [2048], P(('dp', 'tp'))
- grad_query: float32 [2048, 2048], P('dp', 'tp')
- grad_key: float32 [2048, 512], P('dp', 'tp')
- grad_value: float32 [2048, 512], P('dp', 'tp')
- grad_out: float32 [2048, 2048], P('tp', 'dp')
- grad_gain_ffn: float32 [2048], P(('dp', 'tp'))
- grad_gate: float32 [2048, 8192], P('dp', 'tp')
- grad_up: float32 [2048, 8192], P('dp', 'tp')
- grad_down: float32 [8192, 2048], P('tp', 'dp')
The draws below stay inside these ranges and needn't reach their ends.
Inputs may be any that keep to these rules, and one draw needn't show every extreme that they name: Bucket b holds one sequence in its first seq_lens[b] slots; the slots after it are padding. `pad_mask`: every slot after a bucket's sequence is padding; the whole first bucket is live. `positions`: inside a bucket's sequence a token's position counts the live tokens before it; the padding after the sequence has position 0.
All inputs are finite; a program needn't handle non-finite values.
Results may differ from the reference program's by a relative error of at most 0.013.
Values may be sent and summed in bfloat16 or wider, within the bound.
No kernel may reach another device: no remote copies, remote signals or barrier semaphores. Data moves between devices by JAX's collectives and lax.ppermute only.
A program may use at most 256 MiB of HBM per device.

```python
import math
import jax
import jax.numpy as jnp
import numpy as np
from jax import lax

MODEL_WIDTH = 2048
QUERY_HEADS = 32
KEY_VALUE_HEADS = 8
HEAD_SIZE = 64
FF = 8192
GRP = 256
BUCKETS = 16
TOKENS = 4096


def bucket_layout(key):
    length_key = jax.random.fold_in(key, 101)
    mask_key = jax.random.fold_in(key, 202)
    seq_length = jax.random.randint(length_key, (BUCKETS,), GRP // 2, GRP + 1)
    bucket_ids = jnp.arange(BUCKETS)
    seq_length = jnp.where(bucket_ids == 0, GRP, seq_length)
    seq_length = jnp.where(bucket_ids == BUCKETS - 1, GRP // 2, seq_length).astype(jnp.int32)
    live_mask = (jax.random.randint(mask_key, (BUCKETS, GRP), 0, 8) < 7).astype(jnp.int32)
    slot_ids = jnp.arange(GRP)[None, :]
    full_first = (bucket_ids[:, None] == 0) & (slot_ids < GRP)
    live_mask = jnp.where(full_first, 1, live_mask)
    tail_slot = slot_ids >= seq_length[:, None]
    live_mask = jnp.where(tail_slot, 0, live_mask).astype(jnp.int32)
    before = jnp.cumsum(live_mask, axis=1) - live_mask
    position = jnp.where(tail_slot, 0, before).astype(jnp.int32)
    return (seq_length, live_mask.reshape(BUCKETS * GRP), position.reshape(BUCKETS * GRP))


def draw_seq_lens(key, part):
    return bucket_layout(key)[0]


def draw_pad_mask(key, part):
    return bucket_layout(key)[1]


def draw_positions(key, part):
    return bucket_layout(key)[2]


def with_spikes(drawn, key, source, target, shards_of, factor):
    def block_of(dim):
        return (jnp.arange(drawn.shape[dim]) // (drawn.shape[dim] // shards_of)).reshape((-1,) + (1,) * (drawn.ndim - 1 - dim))

    first = jax.random.permutation(key, shards_of)[block_of(target)]
    far = (block_of(target) + shards_of // 2) % shards_of
    return jnp.where((block_of(source) == first) | (block_of(source) == far), factor * drawn, drawn)


def block_scale(stream_key, shape, pieces, least, largest):
    loudness, own = 1.0, jax.random.fold_in(stream_key, 6)
    for dim, blocks in pieces:
        steps = jnp.exp(jax.random.uniform(jax.random.fold_in(own, dim), (blocks,), jnp.float32, least / len(pieces), largest / len(pieces)))
        loudness = loudness * jnp.repeat(steps, shape[dim] // blocks).reshape([-1 if axis == dim else 1 for axis in range(len(shape))])
    return loudness


def noise(stream_key, dims, scale, most, cuts=(), kind=jnp.bfloat16):
    array = jax.random.normal(stream_key, dims, jnp.float32) * scale
    if len(cuts) > 0:
        array = block_scale(stream_key, dims, cuts, -0.22, 0.18) * array
    return jnp.clip(array, min=-most, max=most).astype(kind)


def bell_draw_with(own_key, shape, spread, bound, shards, heavy, held_as=jnp.bfloat16):
    values = spread * jax.random.normal(own_key, shape, jnp.float32)
    if shards:
        values = values * block_scale(own_key, shape, shards, -0.22, 0.18)
    return jnp.clip(with_spikes(values, jax.random.fold_in(own_key, 3), *heavy), -bound, bound).astype(held_as)


def setup_inputs(seed: int = 0) -> dict:
    arg_keys = jax.random.split(jax.random.key(seed), 15)
    tokens = bell_draw_with(arg_keys[0], (TOKENS, MODEL_WIDTH), 1.0, 6.0, ((0, 32),), (0, 1, 32, 2.75))
    gain_attn = jnp.clip(1.0 + 0.1 * jax.random.normal(arg_keys[1], (MODEL_WIDTH,), jnp.float32), 0.5, 1.5).astype(jnp.bfloat16)
    query_weight = noise(arg_keys[2], (MODEL_WIDTH, QUERY_HEADS * HEAD_SIZE), MODEL_WIDTH ** -0.5, 0.125, ((0, 16), (1, 2)))
    key_matrix = noise(arg_keys[3], (MODEL_WIDTH, KEY_VALUE_HEADS * HEAD_SIZE), MODEL_WIDTH ** -0.5, 0.125, ((0, 16), (1, 2)))
    value_matrix = noise(arg_keys[4], (MODEL_WIDTH, KEY_VALUE_HEADS * HEAD_SIZE), MODEL_WIDTH ** -0.5, 0.125, ((0, 16), (1, 2)))
    out_weight = noise(arg_keys[5], (QUERY_HEADS * HEAD_SIZE, MODEL_WIDTH), (QUERY_HEADS * HEAD_SIZE // 64) ** -0.5, 1.0, ((0, 2), (1, 16)))
    gain_ffn = jnp.clip(1.0 + 0.1 * jax.random.normal(arg_keys[6], (MODEL_WIDTH,), jnp.float32), 0.5, 1.5).astype(jnp.bfloat16)
    gate_weight = noise(arg_keys[7], (MODEL_WIDTH, FF), MODEL_WIDTH ** -0.5, 0.125, ((0, 16), (1, 2)))
    up_weight = noise(arg_keys[8], (MODEL_WIDTH, FF), MODEL_WIDTH ** -0.5, 0.125, ((0, 16), (1, 2)))
    down_weight = noise(arg_keys[9], (FF, MODEL_WIDTH), FF ** -0.5, 0.0625, ((0, 2), (1, 16)))
    cotangent = bell_draw_with(arg_keys[10], (TOKENS, MODEL_WIDTH), 1.0, 6.0, ((0, 32),), (0, 1, 32, 2.75))
    seq_lens = draw_seq_lens(jax.random.fold_in(arg_keys[14], 71), 0)
    pad_mask = draw_pad_mask(jax.random.fold_in(arg_keys[14], 71), 0)
    positions = draw_positions(jax.random.fold_in(arg_keys[14], 71), 0)
    return dict(tokens=tokens, gain_attn=gain_attn, query_weight=query_weight, key_matrix=key_matrix, value_matrix=value_matrix, out_weight=out_weight, gain_ffn=gain_ffn, gate_weight=gate_weight, up_weight=up_weight, down_weight=down_weight, cotangent=cotangent, seq_lens=seq_lens, pad_mask=pad_mask, positions=positions)


eps = 1e-05
rope_theta = 500000.0
highest = lax.Precision.HIGHEST

@jax.custom_vjp
def lowered_forward(v):
    return lax.optimization_barrier(v.astype(jnp.bfloat16)).astype(jnp.float32)

@jax.custom_vjp
def lowered_backward(v):
    return v

def low_keep(v):
    return (lowered_forward(v), None)

def low_pass(kept, grad):
    return (grad,)

def back_keep(v):
    return (v, None)

def back_low(kept, grad):
    return (lowered_forward(grad),)
lowered_forward.defvjp(low_keep, low_pass)
lowered_backward.defvjp(back_keep, back_low)

def rope_table(head_dim):
    half_dim = head_dim // 2
    base_freq = 1.0 / rope_theta ** (np.arange(half_dim) * 2.0 / head_dim)
    wavelen = 2.0 * math.pi / base_freq
    smooth = (8192.0 / wavelen - 1.0) / 3.0
    middle = (1.0 - smooth) * base_freq / 32.0 + smooth * base_freq
    return np.where(wavelen > 8192.0, base_freq / 32.0, np.where(wavelen < 2048.0, base_freq, middle))

def root_norm(inputs, gain_vec):
    inverse_rms = lax.rsqrt(lax.optimization_barrier(jnp.mean(inputs * inputs, axis=1, keepdims=True)) + eps)
    return inputs * inverse_rms * gain_vec[None, :]

def rotary_apply(heads, cosine_lookup, sine_lookup, turn):
    half_dim = heads.shape[-1] // 2
    cosine_part = cosine_lookup[:, None, :]
    sine_part = turn * sine_lookup[:, None, :]
    front_half = heads[..., :half_dim]
    back_half = heads[..., half_dim:]
    return jnp.concatenate([front_half * cosine_part - back_half * sine_part, back_half * cosine_part + front_half * sine_part], axis=-1)

def allowed_mask(seq_length, live_mask, slot_count):
    slot_ids = jnp.arange(slot_count, dtype=jnp.int32)
    segment = (slot_ids >= seq_length).astype(jnp.int32)
    same_seq = segment[:, None] == segment[None, :]
    causal = slot_ids[None, :] <= slot_ids[:, None]
    keyed = (live_mask[None, :] == 1) | (slot_ids[:, None] == slot_ids[None, :])
    return same_seq & causal & keyed

def matrix_product(left, right):
    return jnp.dot(left, right, precision=highest)

def block_forward(inputs, gain_attn, query_weight, key_matrix, value_matrix, out_weight, gain_ffn, gate_weight, up_weight, down_weight, allowed, cosine_lookup, sine_lookup):
    count_of_rows = inputs.shape[0]
    score_scale = 1.0 / math.sqrt(HEAD_SIZE)
    attention_normed = lowered_forward(root_norm(inputs, gain_attn))
    query_head_split = rotary_apply(lowered_backward(matrix_product(attention_normed, query_weight)).reshape(count_of_rows, QUERY_HEADS, HEAD_SIZE), cosine_lookup, sine_lookup, 1.0)
    query_head_split = lowered_forward(query_head_split).reshape(count_of_rows, KEY_VALUE_HEADS, QUERY_HEADS // KEY_VALUE_HEADS, HEAD_SIZE)
    key_head_split = lowered_forward(rotary_apply(lowered_backward(matrix_product(attention_normed, key_matrix)).reshape(count_of_rows, KEY_VALUE_HEADS, HEAD_SIZE), cosine_lookup, sine_lookup, 1.0))
    value_head_split = lowered_forward(lowered_backward(matrix_product(attention_normed, value_matrix))).reshape(count_of_rows, KEY_VALUE_HEADS, HEAD_SIZE)
    scores = jnp.einsum('qgmd,kgd->gmqk', query_head_split, key_head_split, precision=highest) * score_scale
    scores = lowered_backward(scores)
    scores = jnp.where(allowed[None, None], scores, -1e+30)
    probs_low = lowered_forward(jax.nn.softmax(scores, axis=-1))
    attended = jnp.einsum('gmqk,kgd->qgmd', probs_low, value_head_split, precision=highest).reshape(count_of_rows, QUERY_HEADS * HEAD_SIZE)
    attended = lowered_forward(lowered_backward(attended))
    resid = inputs + lowered_backward(matrix_product(attended, out_weight))
    normed_ffn = lowered_forward(root_norm(resid, gain_ffn))
    gate_proj = lowered_backward(matrix_product(normed_ffn, gate_weight))
    up_proj = lowered_backward(matrix_product(normed_ffn, up_weight))
    hidden = lowered_forward(jax.nn.silu(gate_proj) * up_proj)
    return resid + matrix_product(hidden, down_weight)

def reference(tokens, gain_attn, query_weight, key_matrix, value_matrix, out_weight, gain_ffn, gate_weight, up_weight, down_weight, cotangent, seq_lens, pad_mask, positions):
    inverse_freq = jnp.asarray(rope_table(HEAD_SIZE), jnp.float32)
    params = tuple((weight.astype(jnp.float32) for weight in (gain_attn, query_weight, key_matrix, value_matrix, out_weight, gain_ffn, gate_weight, up_weight, down_weight)))

    def one_bucket(totals, bucket):
        rows_in, rows_grad, seq_length, live_mask, position = bucket
        angles = position.astype(jnp.float32)[:, None] * inverse_freq[None, :]
        cosine_lookup = jnp.cos(angles)
        sine_lookup = jnp.sin(angles)
        allowed = allowed_mask(seq_length, live_mask, GRP)

        def forward(inputs, *weights):
            return block_forward(inputs, *weights, allowed, cosine_lookup, sine_lookup)
        result, pullback = jax.vjp(forward, rows_in.astype(jnp.float32), *params)
        gradients = pullback(rows_grad.astype(jnp.float32))
        totals = tuple((total + grad_part for total, grad_part in zip(totals, gradients[1:])))
        return (totals, (result.astype(jnp.bfloat16), gradients[0]))
    zero_grads = tuple((jnp.zeros(weight.shape, jnp.float32) for weight in params))
    buckets = (tokens.reshape(BUCKETS, GRP, MODEL_WIDTH), cotangent.reshape(BUCKETS, GRP, MODEL_WIDTH), seq_lens, pad_mask.reshape(BUCKETS, GRP), positions.reshape(BUCKETS, GRP))
    totals, stacked = lax.scan(one_bucket, zero_grads, buckets)
    return (stacked[0].reshape(TOKENS, MODEL_WIDTH), stacked[1].reshape(TOKENS, MODEL_WIDTH), totals[0], totals[1], totals[2], totals[3], totals[4], totals[5], totals[6], totals[7], totals[8])
```

```python
import math

import jax
import jax.numpy as jnp
import numpy as np
from jax import lax
from jax.experimental import pallas as pl
from jax.experimental.pallas import tpu as pltpu
from jax.sharding import PartitionSpec as P

HEAD_SIZE = 64


eps = 1e-05
rope_theta = 500000.0
f32 = jnp.float32
bf16 = jnp.bfloat16


def rope_table(head_dim):
    half_dim = head_dim // 2
    base_freq = 1.0 / rope_theta ** (np.arange(half_dim) * 2.0 / head_dim)
    wavelen = 2.0 * math.pi / base_freq
    smooth = (8192.0 / wavelen - 1.0) / 3.0
    middle = (1.0 - smooth) * base_freq / 32.0 + smooth * base_freq
    return np.where(
        wavelen > 8192.0, base_freq / 32.0, np.where(wavelen < 2048.0, base_freq, middle)
    )


def rotary_apply(heads, cosine_lookup, sine_lookup, turn):
    half_dim = heads.shape[-1] // 2
    cosine_part = cosine_lookup[:, None, :]
    sine_part = turn * sine_lookup[:, None, :]
    front_half = heads[..., :half_dim]
    back_half = heads[..., half_dim:]
    return jnp.concatenate(
        [
            front_half * cosine_part - back_half * sine_part,
            back_half * cosine_part + front_half * sine_part,
        ],
        axis=-1,
    )


def dot(left, right):
    return jnp.dot(left, right, preferred_element_type=f32)


def contract_rows(left, right):
    return lax.dot_general(left, right, (((0,), (0,)), ((), ())), preferred_element_type=f32)


def contract_cols(left, right):
    return lax.dot_general(left, right, (((1,), (1,)), ((), ())), preferred_element_type=f32)


def after(value, *earlier):
    return lax.optimization_barrier((value,) + earlier)[0]


class Axes:
    def __init__(self, dp):
        self.dp = dp
        self.n = dp // 4
        index = lax.axis_index("dp").astype(jnp.int32)
        self.z = index // 4
        self.x = (index // 2) % 2
        self.c = index % 2
        self.y = lax.axis_index("tp").astype(jnp.int32)

    def over_core(self, value):
        return lax.ppermute(value, "dp", [(i, i ^ 1) for i in range(self.dp)])

    def over_x(self, value):
        return lax.ppermute(value, "dp", [(i, i ^ 2) for i in range(self.dp)])

    def over_y(self, value):
        return lax.ppermute(value, "tp", [(0, 1), (1, 0)])

    def over_z(self, value, pairs):
        return lax.ppermute(
            value, "dp", [(a * 4 + low, b * 4 + low) for a, b in pairs for low in range(4)]
        )

    def across(self, step):
        return [(i, i ^ step) for i in range(self.n)]

    def gather_z(self, own):
        if self.n != 4:
            return [own] + [self.over_z(own, self.across(s)) for s in range(1, self.n)]
        one = self.over_z(own, self.across(1))
        three = self.over_z(own, [(1, 2), (2, 1)])
        two_out = self.over_z(three, [(1, 0), (2, 3)])
        two_in = self.over_z(one, [(1, 2), (2, 1)])
        three_out = self.over_z(two_in, [(1, 0), (2, 3)])
        return [own, one, two_out + two_in, three + three_out]

    def scatter_z(self, parts):
        if self.n != 4:
            total = parts[0].astype(f32)
            for s in range(1, self.n):
                total = total + self.over_z(parts[s].astype(bf16), self.across(s)).astype(f32)
            return total
        far = self.over_z(parts[3].astype(bf16), [(0, 1), (3, 2)])
        near = self.over_z(parts[2].astype(bf16), [(0, 1), (3, 2)])
        passed = (parts[2].astype(f32) + far.astype(f32)).astype(bf16)
        passed = self.over_z(passed, [(1, 2), (2, 1)])
        three = (parts[3].astype(f32) + near.astype(f32)).astype(bf16)
        three = self.over_z(three, [(1, 2), (2, 1)])
        one = (parts[1].astype(f32) + passed.astype(f32)).astype(bf16)
        one = self.over_z(one, self.across(1))
        return parts[0].astype(f32) + one.astype(f32) + three.astype(f32)

    def exchange_z(self, parts):
        return [parts[0]] + [self.over_z(parts[s], self.across(s)) for s in range(1, self.n)]

    def place_rows(self, parts):
        count = len(parts)
        rows, cols = parts[0].shape
        tile = min(cols, 512)

        def body(z_ref, *refs):
            for s in range(count):
                refs[-1][z_ref[0] ^ s] = refs[s][...]

        out = pl.pallas_call(
            body,
            out_shape=jax.ShapeDtypeStruct((count, rows, cols), parts[0].dtype),
            grid_spec=pltpu.PrefetchScalarGridSpec(
                num_scalar_prefetch=1,
                grid=(cols // tile,),
                in_specs=[pl.BlockSpec((rows, tile), lambda i, z: (0, i))] * count,
                out_specs=pl.BlockSpec((count, rows, tile), lambda i, z: (0, 0, i)),
            ),
            name="place_rows",
        )(self.z.reshape(1), *parts)
        return out.reshape(count * rows, cols)

    def gather_rows(self, own):
        parts = self.gather_z(own)
        here = self.place_rows(parts)
        there = self.place_rows([self.over_x(part) for part in parts])
        return [here, there, self.over_core(here), self.over_core(there)]

    def reduce_rows(self, left, right):
        width = left.shape[1]
        half, quarter = width // 2, width // 4
        away = contract_rows(left[:, half:], right).astype(bf16)
        got = self.over_core(away)
        beside = (contract_rows(left[:, quarter:half], right) + got[quarter:].astype(f32)).astype(bf16)
        beside_got = self.over_x(beside)
        here = (
            contract_rows(left[:, :quarter], right)
            + got[:quarter].astype(f32)
            + beside_got.astype(f32)
        ).astype(bf16)
        here = here.reshape(self.n, quarter // self.n, right.shape[1])
        return [
            lax.dynamic_index_in_dim(here, self.z ^ s, 0, keepdims=False) for s in range(self.n)
        ]


def finish_ffn(axes, both, down, gain, gate_weight, up_weight):
    count = len(both)
    rows = both[0].shape[0]
    width = both[0].shape[1] // 2

    def body(z_ref, gain_ref, gate_w, up_w, *refs):
        both_refs, down_refs = refs[:count], refs[count : 2 * count]
        gate_out, up_out, down_out, gain_out = refs[2 * count :]
        scale = gain_ref[...]
        total = jnp.zeros((rows, 1), f32)
        for s in range(count):
            start = pl.multiple_of((z_ref[0] ^ s) * width, width)
            spot = pl.ds(start, width)
            gate_part = both_refs[s][:, :width].astype(f32)
            up_part = both_refs[s][:, width:].astype(f32)
            gate_out[:, spot] = gate_part * scale
            up_out[:, spot] = up_part * scale
            total = total + jnp.sum(
                gate_part * gate_w[:, spot].astype(f32) + up_part * up_w[:, spot].astype(f32),
                axis=1,
                keepdims=True,
            )
            down_out[spot, :] = down_refs[s][...].astype(f32).T
        gain_out[...] = total

    full = count * width
    memory = pl.BlockSpec(memory_space=pltpu.VMEM)
    return pl.pallas_call(
        body,
        out_shape=(
            jax.ShapeDtypeStruct((rows, full), f32),
            jax.ShapeDtypeStruct((rows, full), f32),
            jax.ShapeDtypeStruct((full, rows), f32),
            jax.ShapeDtypeStruct((rows, 1), f32),
        ),
        in_specs=[pl.BlockSpec(memory_space=pltpu.SMEM)] + [memory] * (3 + 2 * count),
        out_specs=(memory,) * 4,
        name="finish_ffn",
    )(axes.z.reshape(1), gain, gate_weight, up_weight, *both, *down)


def norm_back(value, inverse, grad):
    mean = jnp.mean(grad * value, axis=1, keepdims=True)
    return inverse * grad - value * (inverse * inverse * inverse * mean)


def shards(
    dp,
    tokens,
    gain_attn,
    query_weight,
    key_matrix,
    value_matrix,
    out_weight,
    gain_ffn,
    gate_weight,
    up_weight,
    down_weight,
    cotangent,
    seq_lens,
    pad_mask,
    positions,
):
    axes = Axes(dp)
    n = axes.n
    own_rows, width = tokens.shape
    block = width // dp
    group_rows = pad_mask.shape[0]
    query_cols = query_weight.shape[1]
    key_cols = key_matrix.shape[1]
    heads_kv = key_cols // HEAD_SIZE
    heads_query = query_cols // HEAD_SIZE
    group_size = heads_query // heads_kv
    score_scale = 1.0 / math.sqrt(HEAD_SIZE)
    hidden_cols = gate_weight.shape[1] // n
    quarter = width // 4

    place = jnp.arange(dp, dtype=jnp.int32)
    to_block = (place % n) * 4 + (((place // n) % 2) ^ axes.x) * 2 + ((place // (2 * n)) ^ axes.c)
    to_place = ((place % 2) ^ axes.c) * (2 * n) + (((place // 2) % 2) ^ axes.x) * n + place // 4

    def reorder(value, order):
        blocks = value.reshape(value.shape[0], dp, block)
        return jnp.take(blocks, order, axis=1, mode="clip").reshape(value.shape)

    scale_attn = gain_attn.astype(f32)[:, None]
    scale_ffn = gain_ffn.astype(f32)[:, None]
    own_qkv = jnp.concatenate([query_weight, key_matrix, value_matrix], axis=1)
    qkv_pieces = axes.gather_rows((own_qkv.astype(f32) * scale_attn).astype(bf16))
    out_pieces = axes.gather_rows(after(out_weight.T, qkv_pieces[0]))

    def hidden_part(weight, s):
        part = lax.dynamic_slice_in_dim(weight, (axes.z ^ s) * hidden_cols, hidden_cols, 1)
        return (part.astype(f32) * scale_ffn).astype(bf16)

    def down_part(s):
        return lax.dynamic_slice_in_dim(
            down_weight, (axes.z ^ s) * hidden_cols, hidden_cols, 0
        ).T

    def gather_hidden(parts):
        here = axes.place_rows(axes.exchange_z(parts))
        there = axes.over_x(here)
        return jnp.concatenate(
            [here, there, axes.over_core(here), axes.over_core(there)], axis=0
        )

    both_parts = [
        jnp.concatenate([hidden_part(gate_weight, s), hidden_part(up_weight, s)], axis=1)
        for s in range(n)
    ]
    down_parts = [down_part(s) for s in range(n)]
    both_full = gather_hidden([after(part, out_pieces[0]) for part in both_parts])
    down_full = gather_hidden([after(part, both_full) for part in down_parts])

    inputs_wide = reorder(tokens, to_block).astype(f32)
    cotangent_low = reorder(cotangent, to_block)
    inverse_one = lax.rsqrt(jnp.mean(inputs_wide * inputs_wide, axis=1, keepdims=True) + eps)
    normed_one = (inputs_wide * inverse_one).astype(bf16)

    def pair_rows(own):
        return jnp.concatenate([own, axes.over_y(own)], axis=0)

    def pair_of(vector):
        halves = vector.reshape(2, own_rows)
        return jnp.concatenate([jnp.take(halves, axes.y, axis=0), jnp.take(halves, 1 - axes.y, axis=0)])

    normed_one_all = pair_rows(normed_one)

    def columns(value, piece):
        return value[:, piece * quarter : (piece + 1) * quarter]

    qkv = sum(dot(columns(normed_one_all, i), qkv_pieces[i]) for i in range(4))
    slot_ids = pair_of(jnp.arange(group_rows, dtype=jnp.int32))
    live_mask = pair_of(pad_mask)
    inverse_freq = jnp.asarray(rope_table(HEAD_SIZE), f32)
    angles = pair_of(positions).astype(f32)[:, None] * inverse_freq[None, :]
    cosine_lookup = jnp.cos(angles)
    sine_lookup = jnp.sin(angles)
    query_head_split = rotary_apply(
        qkv[:, :query_cols].reshape(group_rows, heads_query, HEAD_SIZE),
        cosine_lookup,
        sine_lookup,
        1.0,
    )
    query_head_split = query_head_split.astype(bf16).reshape(
        group_rows, heads_kv, group_size, HEAD_SIZE
    )
    key_head_split = rotary_apply(
        qkv[:, query_cols : query_cols + key_cols].reshape(group_rows, heads_kv, HEAD_SIZE),
        cosine_lookup,
        sine_lookup,
        1.0,
    ).astype(bf16)
    value_head_split = (
        qkv[:, query_cols + key_cols :].astype(bf16).reshape(group_rows, heads_kv, HEAD_SIZE)
    )
    segment = (slot_ids >= seq_lens[0]).astype(jnp.int32)
    allowed = (
        (segment[:, None] == segment[None, :])
        & (slot_ids[None, :] <= slot_ids[:, None])
        & ((live_mask[None, :] == 1) | (slot_ids[:, None] == slot_ids[None, :]))
    )
    scores = (
        jnp.einsum("qgmd,kgd->gmqk", query_head_split, key_head_split, preferred_element_type=f32)
        * score_scale
    )
    scores = jnp.where(allowed[None, None], scores, -1e30)
    row_peak = jnp.max(scores, axis=-1, keepdims=True)
    log_total = row_peak + jnp.log(jnp.sum(jnp.exp(scores - row_peak), axis=-1, keepdims=True))
    probs_low = jnp.exp(scores - log_total).astype(bf16)
    attended = jnp.einsum("gmqk,kgd->qgmd", probs_low, value_head_split, preferred_element_type=f32)
    attended = attended.reshape(group_rows, heads_query * HEAD_SIZE).astype(bf16)

    def split_sum(pieces):
        sent = jnp.concatenate([piece(slice(own_rows, None)) for piece in pieces], axis=1)
        got = axes.over_y(sent.astype(bf16))
        kept = jnp.concatenate([piece(slice(0, own_rows)) for piece in pieces], axis=1)
        return kept + got.astype(f32)

    branch = split_sum(
        [lambda rows, i=i: contract_cols(attended[rows], out_pieces[i]) for i in range(4)]
    )
    resid = inputs_wide + branch
    inverse_two = lax.rsqrt(jnp.mean(resid * resid, axis=1, keepdims=True) + eps)
    normed_two = (resid * inverse_two).astype(bf16)

    def gather_tokens(own):
        parts = axes.gather_z(own)
        return jnp.concatenate(parts + [axes.over_y(part) for part in parts], axis=0)

    normed_two_all = gather_tokens(normed_two)
    cotangent_all = gather_tokens(after(cotangent_low, normed_two_all))
    line_rows = n * own_rows
    gate_up = dot(normed_two_all, both_full)
    gate_proj, up_proj = gate_up[:, :hidden_cols], gate_up[:, hidden_cols:]
    sigmoid_gate = jax.nn.sigmoid(gate_proj)
    gate_active = gate_proj * sigmoid_gate
    hidden = (gate_active * up_proj).astype(bf16)
    hidden_grad = dot(cotangent_all, down_full)
    gate_grad = (
        hidden_grad * up_proj * sigmoid_gate * (1.0 + gate_proj * (1.0 - sigmoid_gate))
    ).astype(bf16)
    up_grad = (hidden_grad * gate_active).astype(bf16)
    both_grad = jnp.concatenate([gate_grad, up_grad], axis=1)

    def scatter_tokens(left, right):
        sent = contract_cols(left[line_rows:], right).astype(bf16)
        got = [
            axes.over_y(sent[s * own_rows : (s + 1) * own_rows]) for s in range(n)
        ]
        kept = contract_cols(left[:line_rows], right)
        return axes.scatter_z(
            [
                kept[s * own_rows : (s + 1) * own_rows] + got[s].astype(f32)
                for s in range(n)
            ]
        )

    normed_two_grad = scatter_tokens(both_grad, both_full)
    branch_feed = scatter_tokens(after(hidden, normed_two_grad), down_full)
    output = reorder((resid + branch_feed).astype(bf16), to_place)

    down_sums = axes.reduce_rows(cotangent_all, hidden)
    both_sums = axes.reduce_rows(normed_two_all, both_grad)
    down_got = axes.exchange_z(down_sums)
    both_got = axes.exchange_z(both_sums)
    grad_gate, grad_up, grad_down, gain_two_sum = finish_ffn(
        axes, both_got, down_got, scale_ffn, gate_weight, up_weight
    )

    resid_grad = cotangent_low.astype(f32) + norm_back(resid, inverse_two, normed_two_grad)
    resid_low_all = pair_rows(resid_grad.astype(bf16))
    attended_grad = sum(dot(columns(resid_low_all, i), out_pieces[i]) for i in range(4))
    out_sum = axes.scatter_z(axes.reduce_rows(resid_low_all, attended))
    attended_heads = attended_grad.astype(bf16).reshape(
        group_rows, heads_kv, group_size, HEAD_SIZE
    )
    probs_full = jnp.exp(scores - log_total)
    prob_grad = jnp.einsum(
        "qgmd,kgd->gmqk", attended_heads, value_head_split, preferred_element_type=f32
    )
    row_delta = jnp.sum(prob_grad * probs_full, axis=-1, keepdims=True)
    score_grad = (probs_full * (prob_grad - row_delta)).astype(bf16)
    value_grad = jnp.einsum("gmqk,qgmd->kgd", probs_low, attended_heads, preferred_element_type=f32)
    value_grad = value_grad.reshape(group_rows, key_cols).astype(bf16)
    query_grad = (
        jnp.einsum("gmqk,kgd->qgmd", score_grad, key_head_split, preferred_element_type=f32)
        * score_scale
    )
    query_grad = rotary_apply(
        query_grad.reshape(group_rows, heads_query, HEAD_SIZE), cosine_lookup, sine_lookup, -1.0
    )
    query_grad = query_grad.reshape(group_rows, query_cols).astype(bf16)
    key_grad = (
        jnp.einsum("gmqk,qgmd->kgd", score_grad, query_head_split, preferred_element_type=f32)
        * score_scale
    )
    key_grad = (
        rotary_apply(key_grad, cosine_lookup, sine_lookup, -1.0)
        .reshape(group_rows, key_cols)
        .astype(bf16)
    )
    qkv_grad = jnp.concatenate([query_grad, key_grad, value_grad], axis=1)
    normed_one_grad = split_sum(
        [lambda rows, i=i: contract_cols(qkv_grad[rows], qkv_pieces[i]) for i in range(4)]
    )
    qkv_sum = axes.scatter_z(axes.reduce_rows(normed_one_all, qkv_grad))
    token_grad = reorder(
        resid_grad + norm_back(inputs_wide, inverse_one, normed_one_grad), to_place
    )
    gain_one_sum = jnp.sum(qkv_sum * own_qkv.astype(f32), axis=1)
    qkv_out = qkv_sum * scale_attn

    def share(vector):
        total = vector + axes.over_y(vector)
        return lax.dynamic_slice_in_dim(total, axes.y * (block // 2), block // 2)

    return (
        output,
        token_grad,
        share(gain_one_sum),
        qkv_out[:, :query_cols],
        qkv_out[:, query_cols : query_cols + key_cols],
        qkv_out[:, query_cols + key_cols :],
        out_sum.T,
        share(gain_two_sum[:, 0]),
        grad_gate,
        grad_up,
        grad_down,
    )


def solution(mesh):
    dp = mesh.shape["dp"]
    placed = (
        P(("dp", "tp"), None),
        P("dp"),
        P("dp", "tp"),
        P("dp", "tp"),
        P("dp", "tp"),
        P("tp", "dp"),
        P("dp"),
        P("dp", "tp"),
        P("dp", "tp"),
        P("tp", "dp"),
        P(("dp", "tp"), None),
        P("dp"),
        P("dp"),
        P("dp"),
    )

    def program(*arrays):
        return shards(dp, *arrays)

    return jax.shard_map(
        program,
        mesh=mesh,
        in_specs=placed,
        out_specs=(
            P(("dp", "tp"), None),
            P(("dp", "tp"), None),
            P(("dp", "tp")),
            P("dp", "tp"),
            P("dp", "tp"),
            P("dp", "tp"),
            P("tp", "dp"),
            P(("dp", "tp")),
            P("dp", "tp"),
            P("dp", "tp"),
            P("tp", "dp"),
        ),
        check_vma=False,
    )
```

```python
import math

import jax
import jax.numpy as jnp
import numpy as np
from jax import lax
from jax.experimental import pallas as pl
from jax.experimental.pallas import tpu as pltpu
from jax.sharding import PartitionSpec as P

HEAD_SIZE = 64


eps = 1e-05
rope_theta = 500000.0
f32 = jnp.float32
bf16 = jnp.bfloat16


def rope_table(head_dim):
    half_dim = head_dim // 2
    base_freq = 1.0 / rope_theta ** (np.arange(half_dim) * 2.0 / head_dim)
    wavelen = 2.0 * math.pi / base_freq
    smooth = (8192.0 / wavelen - 1.0) / 3.0
    middle = (1.0 - smooth) * base_freq / 32.0 + smooth * base_freq
    return np.where(
        wavelen > 8192.0, base_freq / 32.0, np.where(wavelen < 2048.0, base_freq, middle)
    )


def rotary_apply(heads, cosine_lookup, sine_lookup, turn):
    half_dim = heads.shape[-1] // 2
    cosine_part = cosine_lookup[:, None, :]
    sine_part = turn * sine_lookup[:, None, :]
    front_half = heads[..., :half_dim]
    back_half = heads[..., half_dim:]
    return jnp.concatenate(
        [
            front_half * cosine_part - back_half * sine_part,
            back_half * cosine_part + front_half * sine_part,
        ],
        axis=-1,
    )


def dot(left, right):
    return jnp.dot(left, right, preferred_element_type=f32)


def contract_rows(left, right):
    return lax.dot_general(left, right, (((0,), (0,)), ((), ())), preferred_element_type=f32)


def contract_cols(left, right):
    return lax.dot_general(left, right, (((1,), (1,)), ((), ())), preferred_element_type=f32)


def after(value, *earlier):
    return lax.optimization_barrier((value,) + earlier)[0]


class Axes:
    def __init__(self, dp):
        self.dp = dp
        self.n = dp // 4
        index = lax.axis_index("dp").astype(jnp.int32)
        self.z = index // 4
        self.x = (index // 2) % 2
        self.c = index % 2
        self.y = lax.axis_index("tp").astype(jnp.int32)

    def over_core(self, value):
        return lax.ppermute(value, "dp", [(i, i ^ 1) for i in range(self.dp)])

    def over_x(self, value):
        return lax.ppermute(value, "dp", [(i, i ^ 2) for i in range(self.dp)])

    def over_y(self, value):
        return lax.ppermute(value, "tp", [(0, 1), (1, 0)])

    def over_z(self, value, pairs):
        return lax.ppermute(
            value, "dp", [(a * 4 + low, b * 4 + low) for a, b in pairs for low in range(4)]
        )

    def across(self, step):
        return [(i, i ^ step) for i in range(self.n)]

    def gather_z(self, own):
        if self.n != 4:
            return [own] + [self.over_z(own, self.across(s)) for s in range(1, self.n)]
        one = self.over_z(own, self.across(1))
        three = self.over_z(own, [(1, 2), (2, 1)])
        two_out = self.over_z(three, [(1, 0), (2, 3)])
        two_in = self.over_z(one, [(1, 2), (2, 1)])
        three_out = self.over_z(two_in, [(1, 0), (2, 3)])
        return [own, one, two_out + two_in, three + three_out]

    def scatter_z(self, parts):
        if self.n != 4:
            total = parts[0].astype(f32)
            for s in range(1, self.n):
                total = total + self.over_z(parts[s].astype(bf16), self.across(s)).astype(f32)
            return total
        far = self.over_z(parts[3].astype(bf16), [(0, 1), (3, 2)])
        near = self.over_z(parts[2].astype(bf16), [(0, 1), (3, 2)])
        passed = (parts[2].astype(f32) + far.astype(f32)).astype(bf16)
        passed = self.over_z(passed, [(1, 2), (2, 1)])
        three = (parts[3].astype(f32) + near.astype(f32)).astype(bf16)
        three = self.over_z(three, [(1, 2), (2, 1)])
        one = (parts[1].astype(f32) + passed.astype(f32)).astype(bf16)
        one = self.over_z(one, self.across(1))
        return parts[0].astype(f32) + one.astype(f32) + three.astype(f32)

    def exchange_z(self, parts):
        return [parts[0]] + [self.over_z(parts[s], self.across(s)) for s in range(1, self.n)]

    def place_rows(self, parts):
        count = len(parts)
        rows, cols = parts[0].shape
        tile = min(cols, 512)

        def body(z_ref, *refs):
            for s in range(count):
                refs[-1][z_ref[0] ^ s] = refs[s][...]

        out = pl.pallas_call(
            body,
            out_shape=jax.ShapeDtypeStruct((count, rows, cols), parts[0].dtype),
            grid_spec=pltpu.PrefetchScalarGridSpec(
                num_scalar_prefetch=1,
                grid=(cols // tile,),
                in_specs=[pl.BlockSpec((rows, tile), lambda i, z: (0, i))] * count,
                out_specs=pl.BlockSpec((count, rows, tile), lambda i, z: (0, 0, i)),
            ),
            name="place_rows",
        )(self.z.reshape(1), *parts)
        return out.reshape(count * rows, cols)

    def gather_rows(self, own):
        parts = self.gather_z(own)
        here = self.place_rows(parts)
        there = self.place_rows([self.over_x(part) for part in parts])
        return [here, there, self.over_core(here), self.over_core(there)]

    def reduce_rows(self, left, right, *earlier):
        width = left.shape[1]
        half, quarter = width // 2, width // 4
        away = contract_rows(left[:, half:], right).astype(bf16)
        got = self.over_core(away)
        beside = (contract_rows(left[:, quarter:half], right) + got[quarter:].astype(f32)).astype(bf16)
        beside_got = self.over_x(beside)
        if earlier:
            beside_got = after(beside_got, *earlier)
        here = (
            contract_rows(left[:, :quarter], right)
            + got[:quarter].astype(f32)
            + beside_got.astype(f32)
        ).astype(bf16)
        here = here.reshape(self.n, quarter // self.n, right.shape[1])
        parts = [
            lax.dynamic_index_in_dim(here, self.z ^ s, 0, keepdims=False) for s in range(self.n)
        ]
        return parts, beside


def finish_ffn(axes, both, down, gain, gate_weight, up_weight):
    count = len(both)
    rows = both[0].shape[0]
    width = both[0].shape[1] // 2

    def body(z_ref, gain_ref, gate_w, up_w, *refs):
        both_refs, down_refs = refs[:count], refs[count : 2 * count]
        gate_out, up_out, down_out, gain_out = refs[2 * count :]
        scale = gain_ref[...]
        total = jnp.zeros((rows, 1), f32)
        for s in range(count):
            start = pl.multiple_of((z_ref[0] ^ s) * width, width)
            spot = pl.ds(start, width)
            gate_part = both_refs[s][:, :width].astype(f32)
            up_part = both_refs[s][:, width:].astype(f32)
            gate_out[:, spot] = gate_part * scale
            up_out[:, spot] = up_part * scale
            total = total + jnp.sum(
                gate_part * gate_w[:, spot].astype(f32) + up_part * up_w[:, spot].astype(f32),
                axis=1,
                keepdims=True,
            )
            down_out[spot, :] = down_refs[s][...].astype(f32).T
        gain_out[...] = total

    full = count * width
    memory = pl.BlockSpec(memory_space=pltpu.VMEM)
    return pl.pallas_call(
        body,
        out_shape=(
            jax.ShapeDtypeStruct((rows, full), f32),
            jax.ShapeDtypeStruct((rows, full), f32),
            jax.ShapeDtypeStruct((full, rows), f32),
            jax.ShapeDtypeStruct((rows, 1), f32),
        ),
        in_specs=[pl.BlockSpec(memory_space=pltpu.SMEM)] + [memory] * (3 + 2 * count),
        out_specs=(memory,) * 4,
        name="finish_ffn",
    )(axes.z.reshape(1), gain, gate_weight, up_weight, *both, *down)


def norm_back(value, inverse, grad):
    mean = jnp.mean(grad * value, axis=1, keepdims=True)
    return inverse * grad - value * (inverse * inverse * inverse * mean)


def shards(
    dp,
    tokens,
    gain_attn,
    query_weight,
    key_matrix,
    value_matrix,
    out_weight,
    gain_ffn,
    gate_weight,
    up_weight,
    down_weight,
    cotangent,
    seq_lens,
    pad_mask,
    positions,
):
    axes = Axes(dp)
    n = axes.n
    own_rows, width = tokens.shape
    block = width // dp
    group_rows = pad_mask.shape[0]
    query_cols = query_weight.shape[1]
    key_cols = key_matrix.shape[1]
    heads_kv = key_cols // HEAD_SIZE
    heads_query = query_cols // HEAD_SIZE
    group_size = heads_query // heads_kv
    score_scale = 1.0 / math.sqrt(HEAD_SIZE)
    hidden_cols = gate_weight.shape[1] // n
    quarter = width // 4

    place = jnp.arange(dp, dtype=jnp.int32)
    to_block = (place % n) * 4 + (((place // n) % 2) ^ axes.x) * 2 + ((place // (2 * n)) ^ axes.c)
    to_place = ((place % 2) ^ axes.c) * (2 * n) + (((place // 2) % 2) ^ axes.x) * n + place // 4

    def reorder(value, order):
        blocks = value.reshape(value.shape[0], dp, block)
        return jnp.take(blocks, order, axis=1, mode="clip").reshape(value.shape)

    scale_attn = gain_attn.astype(f32)[:, None]
    scale_ffn = gain_ffn.astype(f32)[:, None]
    own_qkv = jnp.concatenate([query_weight, key_matrix, value_matrix], axis=1)
    qkv_pieces = axes.gather_rows((own_qkv.astype(f32) * scale_attn).astype(bf16))
    out_pieces = axes.gather_rows(after(out_weight.T, qkv_pieces[0]))

    def hidden_part(weight, s):
        part = lax.dynamic_slice_in_dim(weight, (axes.z ^ s) * hidden_cols, hidden_cols, 1)
        return (part.astype(f32) * scale_ffn).astype(bf16)

    def down_part(s):
        return lax.dynamic_slice_in_dim(
            down_weight, (axes.z ^ s) * hidden_cols, hidden_cols, 0
        ).T

    def gather_hidden(parts):
        here = axes.place_rows(parts)
        there = axes.over_x(here)
        return jnp.concatenate(
            [here, there, axes.over_core(here), axes.over_core(there)], axis=0
        )

    both_parts = [
        jnp.concatenate([hidden_part(gate_weight, s), hidden_part(up_weight, s)], axis=1)
        for s in range(n)
    ]
    down_parts = [down_part(s) for s in range(n)]
    both_got = axes.exchange_z([after(part, out_pieces[0]) for part in both_parts])

    inputs_wide = reorder(tokens, to_block).astype(f32)
    cotangent_low = reorder(cotangent, to_block)
    inverse_one = lax.rsqrt(jnp.mean(inputs_wide * inputs_wide, axis=1, keepdims=True) + eps)
    normed_one = (inputs_wide * inverse_one).astype(bf16)

    def pair_rows(own):
        return jnp.concatenate([own, axes.over_y(own)], axis=0)

    def pair_of(vector):
        halves = vector.reshape(2, own_rows)
        return jnp.concatenate([jnp.take(halves, axes.y, axis=0), jnp.take(halves, 1 - axes.y, axis=0)])

    normed_one_all = pair_rows(normed_one)

    def columns(value, piece):
        return value[:, piece * quarter : (piece + 1) * quarter]

    qkv = sum(dot(columns(normed_one_all, i), qkv_pieces[i]) for i in range(4))
    slot_ids = pair_of(jnp.arange(group_rows, dtype=jnp.int32))
    live_mask = pair_of(pad_mask)
    inverse_freq = jnp.asarray(rope_table(HEAD_SIZE), f32)
    angles = pair_of(positions).astype(f32)[:, None] * inverse_freq[None, :]
    cosine_lookup = jnp.cos(angles)
    sine_lookup = jnp.sin(angles)
    query_head_split = rotary_apply(
        qkv[:, :query_cols].reshape(group_rows, heads_query, HEAD_SIZE),
        cosine_lookup,
        sine_lookup,
        1.0,
    )
    query_head_split = query_head_split.astype(bf16).reshape(
        group_rows, heads_kv, group_size, HEAD_SIZE
    )
    key_head_split = rotary_apply(
        qkv[:, query_cols : query_cols + key_cols].reshape(group_rows, heads_kv, HEAD_SIZE),
        cosine_lookup,
        sine_lookup,
        1.0,
    ).astype(bf16)
    value_head_split = (
        qkv[:, query_cols + key_cols :].astype(bf16).reshape(group_rows, heads_kv, HEAD_SIZE)
    )
    segment = (slot_ids >= seq_lens[0]).astype(jnp.int32)
    allowed = (
        (segment[:, None] == segment[None, :])
        & (slot_ids[None, :] <= slot_ids[:, None])
        & ((live_mask[None, :] == 1) | (slot_ids[:, None] == slot_ids[None, :]))
    )
    scores = (
        jnp.einsum("qgmd,kgd->gmqk", query_head_split, key_head_split, preferred_element_type=f32)
        * score_scale
    )
    scores = jnp.where(allowed[None, None], scores, -1e30)
    row_peak = jnp.max(scores, axis=-1, keepdims=True)
    log_total = row_peak + jnp.log(jnp.sum(jnp.exp(scores - row_peak), axis=-1, keepdims=True))
    probs_low = jnp.exp(scores - log_total).astype(bf16)
    attended = jnp.einsum("gmqk,kgd->qgmd", probs_low, value_head_split, preferred_element_type=f32)
    attended = attended.reshape(group_rows, heads_query * HEAD_SIZE).astype(bf16)
    both_full = gather_hidden([after(part, attended) for part in both_got])
    down_full = gather_hidden(axes.exchange_z([after(part, both_full) for part in down_parts]))

    def split_sum(pieces):
        sent = jnp.concatenate([piece(slice(own_rows, None)) for piece in pieces], axis=1)
        got = axes.over_y(sent.astype(bf16))
        kept = jnp.concatenate([piece(slice(0, own_rows)) for piece in pieces], axis=1)
        return kept + got.astype(f32)

    branch = split_sum(
        [lambda rows, i=i: contract_cols(attended[rows], out_pieces[i]) for i in range(4)]
    )
    resid = inputs_wide + branch
    inverse_two = lax.rsqrt(jnp.mean(resid * resid, axis=1, keepdims=True) + eps)
    normed_two = (resid * inverse_two).astype(bf16)

    def gather_tokens(own):
        parts = axes.gather_z(own)
        return jnp.concatenate(parts + [axes.over_y(part) for part in parts], axis=0)

    normed_two_all = gather_tokens(normed_two)
    cotangent_all = gather_tokens(after(cotangent_low, normed_two_all))
    line_rows = n * own_rows
    gate_up = dot(normed_two_all, both_full)
    gate_proj, up_proj = gate_up[:, :hidden_cols], gate_up[:, hidden_cols:]
    sigmoid_gate = jax.nn.sigmoid(gate_proj)
    gate_active = gate_proj * sigmoid_gate
    hidden = (gate_active * up_proj).astype(bf16)
    hidden_grad = dot(cotangent_all, down_full)
    gate_grad = (
        hidden_grad * up_proj * sigmoid_gate * (1.0 + gate_proj * (1.0 - sigmoid_gate))
    ).astype(bf16)
    up_grad = (hidden_grad * gate_active).astype(bf16)
    both_grad = jnp.concatenate([gate_grad, up_grad], axis=1)

    def scatter_tokens(left, right):
        sent = contract_cols(left[line_rows:], right).astype(bf16)
        got = [
            axes.over_y(sent[s * own_rows : (s + 1) * own_rows]) for s in range(n)
        ]
        kept = contract_cols(left[:line_rows], right)
        total = axes.scatter_z(
            [
                kept[s * own_rows : (s + 1) * own_rows] + got[s].astype(f32)
                for s in range(n)
            ]
        )
        return total, got[0]

    normed_two_grad, _ = scatter_tokens(both_grad, both_full)
    branch_feed, feed_got = scatter_tokens(after(hidden, normed_two_grad), down_full)
    output = reorder((resid + branch_feed).astype(bf16), to_place)

    down_sums, _ = axes.reduce_rows(cotangent_all, hidden)
    both_sums, both_beside = axes.reduce_rows(normed_two_all, both_grad)
    down_got = axes.exchange_z(down_sums)
    both_got = axes.exchange_z(both_sums)
    grad_gate, grad_up, grad_down, gain_two_sum = finish_ffn(
        axes, both_got, down_got, scale_ffn, gate_weight, up_weight
    )

    resid_grad = cotangent_low.astype(f32) + norm_back(resid, inverse_two, normed_two_grad)
    resid_low_all = pair_rows(resid_grad.astype(bf16))
    attended_grad = sum(dot(columns(resid_low_all, i), out_pieces[i]) for i in range(4))
    out_sum = axes.scatter_z(
        axes.reduce_rows(resid_low_all, attended, both_sums[1], *down_got[1:])[0]
    )
    attended_heads = attended_grad.astype(bf16).reshape(
        group_rows, heads_kv, group_size, HEAD_SIZE
    )
    probs_full = jnp.exp(scores - log_total)
    prob_grad = jnp.einsum(
        "qgmd,kgd->gmqk", attended_heads, value_head_split, preferred_element_type=f32
    )
    row_delta = jnp.sum(prob_grad * probs_full, axis=-1, keepdims=True)
    score_grad = after((probs_full * (prob_grad - row_delta)).astype(bf16), both_beside, feed_got)
    value_grad = jnp.einsum("gmqk,qgmd->kgd", probs_low, attended_heads, preferred_element_type=f32)
    value_grad = value_grad.reshape(group_rows, key_cols).astype(bf16)
    query_grad = (
        jnp.einsum("gmqk,kgd->qgmd", score_grad, key_head_split, preferred_element_type=f32)
        * score_scale
    )
    query_grad = rotary_apply(
        query_grad.reshape(group_rows, heads_query, HEAD_SIZE), cosine_lookup, sine_lookup, -1.0
    )
    query_grad = query_grad.reshape(group_rows, query_cols).astype(bf16)
    key_grad = (
        jnp.einsum("gmqk,qgmd->kgd", score_grad, query_head_split, preferred_element_type=f32)
        * score_scale
    )
    key_grad = (
        rotary_apply(key_grad, cosine_lookup, sine_lookup, -1.0)
        .reshape(group_rows, key_cols)
        .astype(bf16)
    )
    qkv_grad = jnp.concatenate([query_grad, key_grad, value_grad], axis=1)
    normed_one_grad = split_sum(
        [lambda rows, i=i: contract_cols(qkv_grad[rows], qkv_pieces[i]) for i in range(4)]
    )
    qkv_sum = axes.scatter_z(axes.reduce_rows(normed_one_all, qkv_grad)[0])
    token_grad = reorder(
        resid_grad + norm_back(inputs_wide, inverse_one, normed_one_grad), to_place
    )
    gain_one_sum = jnp.sum(qkv_sum * own_qkv.astype(f32), axis=1)
    qkv_out = qkv_sum * scale_attn

    def share(vector):
        total = vector + axes.over_y(vector)
        return lax.dynamic_slice_in_dim(total, axes.y * (block // 2), block // 2)

    return (
        output,
        token_grad,
        share(gain_one_sum),
        qkv_out[:, :query_cols],
        qkv_out[:, query_cols : query_cols + key_cols],
        qkv_out[:, query_cols + key_cols :],
        out_sum.T,
        share(gain_two_sum[:, 0]),
        grad_gate,
        grad_up,
        grad_down,
    )


def solution(mesh):
    dp = mesh.shape["dp"]
    placed = (
        P(("dp", "tp"), None),
        P("dp"),
        P("dp", "tp"),
        P("dp", "tp"),
        P("dp", "tp"),
        P("tp", "dp"),
        P("dp"),
        P("dp", "tp"),
        P("dp", "tp"),
        P("tp", "dp"),
        P(("dp", "tp"), None),
        P("dp"),
        P("dp"),
        P("dp"),
    )

    def program(*arrays):
        return shards(dp, *arrays)

    return jax.shard_map(
        program,
        mesh=mesh,
        in_specs=placed,
        out_specs=(
            P(("dp", "tp"), None),
            P(("dp", "tp"), None),
            P(("dp", "tp")),
            P("dp", "tp"),
            P("dp", "tp"),
            P("dp", "tp"),
            P("tp", "dp"),
            P(("dp", "tp")),
            P("dp", "tp"),
            P("dp", "tp"),
            P("tp", "dp"),
        ),
        check_vma=False,
    )
```

```python
import math

import jax
import jax.numpy as jnp
import numpy as np
from jax import lax
from jax.experimental import pallas as pl
from jax.experimental.pallas import tpu as pltpu
from jax.sharding import PartitionSpec as P

HEAD_SIZE = 64


eps = 1e-05
rope_theta = 500000.0
f32 = jnp.float32
bf16 = jnp.bfloat16


def rope_table(head_dim):
    half_dim = head_dim // 2
    base_freq = 1.0 / rope_theta ** (np.arange(half_dim) * 2.0 / head_dim)
    wavelen = 2.0 * math.pi / base_freq
    smooth = (8192.0 / wavelen - 1.0) / 3.0
    middle = (1.0 - smooth) * base_freq / 32.0 + smooth * base_freq
    return np.where(
        wavelen > 8192.0, base_freq / 32.0, np.where(wavelen < 2048.0, base_freq, middle)
    )


def rotary_apply(heads, cosine_lookup, sine_lookup, turn):
    half_dim = heads.shape[-1] // 2
    cosine_part = cosine_lookup[:, None, :]
    sine_part = turn * sine_lookup[:, None, :]
    front_half = heads[..., :half_dim]
    back_half = heads[..., half_dim:]
    return jnp.concatenate(
        [
            front_half * cosine_part - back_half * sine_part,
            back_half * cosine_part + front_half * sine_part,
        ],
        axis=-1,
    )


def dot(left, right):
    return jnp.dot(left, right, preferred_element_type=f32)


def contract_rows(left, right):
    return lax.dot_general(left, right, (((0,), (0,)), ((), ())), preferred_element_type=f32)


def contract_cols(left, right):
    return lax.dot_general(left, right, (((1,), (1,)), ((), ())), preferred_element_type=f32)


def after(value, *earlier):
    return lax.optimization_barrier((value,) + earlier)[0]


class Axes:
    def __init__(self, dp):
        self.dp = dp
        self.n = dp // 4
        index = lax.axis_index("dp").astype(jnp.int32)
        self.z = index // 4
        self.x = (index // 2) % 2
        self.c = index % 2
        self.y = lax.axis_index("tp").astype(jnp.int32)

    def over_core(self, value):
        return lax.ppermute(value, "dp", [(i, i ^ 1) for i in range(self.dp)])

    def over_x(self, value):
        return lax.ppermute(value, "dp", [(i, i ^ 2) for i in range(self.dp)])

    def over_y(self, value):
        return lax.ppermute(value, "tp", [(0, 1), (1, 0)])

    def over_z(self, value, pairs):
        return lax.ppermute(
            value, "dp", [(a * 4 + low, b * 4 + low) for a, b in pairs for low in range(4)]
        )

    def across(self, step):
        return [(i, i ^ step) for i in range(self.n)]

    def gather_z(self, own):
        if self.n != 4:
            return [own] + [self.over_z(own, self.across(s)) for s in range(1, self.n)]
        one = self.over_z(own, self.across(1))
        three = self.over_z(own, [(1, 2), (2, 1)])
        two_out = self.over_z(three, [(1, 0), (2, 3)])
        two_in = self.over_z(one, [(1, 2), (2, 1)])
        three_out = self.over_z(two_in, [(1, 0), (2, 3)])
        return [own, one, two_out + two_in, three + three_out]

    def scatter_z(self, parts):
        if self.n != 4:
            total = parts[0].astype(f32)
            for s in range(1, self.n):
                total = total + self.over_z(parts[s].astype(bf16), self.across(s)).astype(f32)
            return total
        far = self.over_z(parts[3].astype(bf16), [(0, 1), (3, 2)])
        near = self.over_z(parts[2].astype(bf16), [(0, 1), (3, 2)])
        passed = (parts[2].astype(f32) + far.astype(f32)).astype(bf16)
        passed = self.over_z(passed, [(1, 2), (2, 1)])
        three = (parts[3].astype(f32) + near.astype(f32)).astype(bf16)
        three = self.over_z(three, [(1, 2), (2, 1)])
        one = (parts[1].astype(f32) + passed.astype(f32)).astype(bf16)
        one = self.over_z(one, self.across(1))
        return parts[0].astype(f32) + one.astype(f32) + three.astype(f32)

    def exchange_z(self, parts):
        return [parts[0]] + [self.over_z(parts[s], self.across(s)) for s in range(1, self.n)]

    def place_rows(self, parts):
        count = len(parts)
        rows, cols = parts[0].shape
        tile = min(cols, 512)

        def body(z_ref, *refs):
            for s in range(count):
                refs[-1][z_ref[0] ^ s] = refs[s][...]

        out = pl.pallas_call(
            body,
            out_shape=jax.ShapeDtypeStruct((count, rows, cols), parts[0].dtype),
            grid_spec=pltpu.PrefetchScalarGridSpec(
                num_scalar_prefetch=1,
                grid=(cols // tile,),
                in_specs=[pl.BlockSpec((rows, tile), lambda i, z: (0, i))] * count,
                out_specs=pl.BlockSpec((count, rows, tile), lambda i, z: (0, 0, i)),
            ),
            name="place_rows",
        )(self.z.reshape(1), *parts)
        return out.reshape(count * rows, cols)

    def gather_rows(self, own):
        parts = self.gather_z(own)
        here = self.place_rows(parts)
        there = self.place_rows([self.over_x(part) for part in parts])
        return [here, there, self.over_core(here), self.over_core(there)]

    def reduce_rows(self, left, right, *earlier):
        width = left.shape[1]
        half, quarter = width // 2, width // 4
        away = contract_rows(left[:, half:], right).astype(bf16)
        got = self.over_core(away)
        beside = (contract_rows(left[:, quarter:half], right) + got[quarter:].astype(f32)).astype(bf16)
        beside_got = self.over_x(beside)
        if earlier:
            beside_got = after(beside_got, *earlier)
        here = (
            contract_rows(left[:, :quarter], right)
            + got[:quarter].astype(f32)
            + beside_got.astype(f32)
        ).astype(bf16)
        here = here.reshape(self.n, quarter // self.n, right.shape[1])
        parts = [
            lax.dynamic_index_in_dim(here, self.z ^ s, 0, keepdims=False) for s in range(self.n)
        ]
        return parts, beside


def finish_ffn(axes, both, down, gain, gate_weight, up_weight):
    count = len(both)
    rows = both[0].shape[0]
    width = both[0].shape[1] // 2

    def body(z_ref, gain_ref, gate_w, up_w, *refs):
        both_refs, down_refs = refs[:count], refs[count : 2 * count]
        gate_out, up_out, down_out, gain_out = refs[2 * count :]
        scale = gain_ref[...]
        total = jnp.zeros((rows, 1), f32)
        for s in range(count):
            start = pl.multiple_of((z_ref[0] ^ s) * width, width)
            spot = pl.ds(start, width)
            gate_part = both_refs[s][:, :width].astype(f32)
            up_part = both_refs[s][:, width:].astype(f32)
            gate_out[:, spot] = gate_part * scale
            up_out[:, spot] = up_part * scale
            total = total + jnp.sum(
                gate_part * gate_w[:, spot].astype(f32) + up_part * up_w[:, spot].astype(f32),
                axis=1,
                keepdims=True,
            )
            down_out[spot, :] = down_refs[s][...].astype(f32).T
        gain_out[...] = total

    full = count * width
    memory = pl.BlockSpec(memory_space=pltpu.VMEM)
    return pl.pallas_call(
        body,
        out_shape=(
            jax.ShapeDtypeStruct((rows, full), f32),
            jax.ShapeDtypeStruct((rows, full), f32),
            jax.ShapeDtypeStruct((full, rows), f32),
            jax.ShapeDtypeStruct((rows, 1), f32),
        ),
        in_specs=[pl.BlockSpec(memory_space=pltpu.SMEM)] + [memory] * (3 + 2 * count),
        out_specs=(memory,) * 4,
        name="finish_ffn",
    )(axes.z.reshape(1), gain, gate_weight, up_weight, *both, *down)


def norm_back(value, inverse, grad):
    mean = jnp.mean(grad * value, axis=1, keepdims=True)
    return inverse * grad - value * (inverse * inverse * inverse * mean)


def shards(
    dp,
    tokens,
    gain_attn,
    query_weight,
    key_matrix,
    value_matrix,
    out_weight,
    gain_ffn,
    gate_weight,
    up_weight,
    down_weight,
    cotangent,
    seq_lens,
    pad_mask,
    positions,
):
    axes = Axes(dp)
    n = axes.n
    own_rows, width = tokens.shape
    block = width // dp
    group_rows = pad_mask.shape[0]
    query_cols = query_weight.shape[1]
    key_cols = key_matrix.shape[1]
    heads_kv = key_cols // HEAD_SIZE
    heads_query = query_cols // HEAD_SIZE
    group_size = heads_query // heads_kv
    score_scale = 1.0 / math.sqrt(HEAD_SIZE)
    hidden_cols = gate_weight.shape[1] // n
    quarter = width // 4

    place = jnp.arange(dp, dtype=jnp.int32)
    to_block = (place % n) * 4 + (((place // n) % 2) ^ axes.x) * 2 + ((place // (2 * n)) ^ axes.c)
    to_place = ((place % 2) ^ axes.c) * (2 * n) + (((place // 2) % 2) ^ axes.x) * n + place // 4

    def reorder(value, order):
        blocks = value.reshape(value.shape[0], dp, block)
        return jnp.take(blocks, order, axis=1, mode="clip").reshape(value.shape)

    scale_attn = gain_attn.astype(f32)[:, None]
    scale_ffn = gain_ffn.astype(f32)[:, None]
    own_qkv = jnp.concatenate([query_weight, key_matrix, value_matrix], axis=1)
    qkv_pieces = axes.gather_rows((own_qkv.astype(f32) * scale_attn).astype(bf16))
    out_pieces = axes.gather_rows(after(out_weight.T, qkv_pieces[0]))

    def hidden_part(weight, s):
        part = lax.dynamic_slice_in_dim(weight, (axes.z ^ s) * hidden_cols, hidden_cols, 1)
        return (part.astype(f32) * scale_ffn).astype(bf16)

    def down_part(s):
        return lax.dynamic_slice_in_dim(
            down_weight, (axes.z ^ s) * hidden_cols, hidden_cols, 0
        ).T

    def gather_hidden(parts):
        here = axes.place_rows(parts)
        there = axes.over_x(here)
        return jnp.concatenate(
            [here, there, axes.over_core(here), axes.over_core(there)], axis=0
        )

    both_parts = [
        jnp.concatenate([hidden_part(gate_weight, s), hidden_part(up_weight, s)], axis=1)
        for s in range(n)
    ]
    down_parts = [down_part(s) for s in range(n)]
    both_got = axes.exchange_z([after(part, out_pieces[0]) for part in both_parts])

    inputs_wide = reorder(tokens, to_block).astype(f32)
    cotangent_low = reorder(cotangent, to_block)
    inverse_one = lax.rsqrt(jnp.mean(inputs_wide * inputs_wide, axis=1, keepdims=True) + eps)
    normed_one = (inputs_wide * inverse_one).astype(bf16)

    def pair_rows(own):
        return jnp.concatenate([own, axes.over_y(own)], axis=0)

    def pair_of(vector):
        halves = vector.reshape(2, own_rows)
        return jnp.concatenate([jnp.take(halves, axes.y, axis=0), jnp.take(halves, 1 - axes.y, axis=0)])

    normed_one_all = pair_rows(normed_one)

    def columns(value, piece):
        return value[:, piece * quarter : (piece + 1) * quarter]

    qkv = sum(dot(columns(normed_one_all, i), qkv_pieces[i]) for i in range(4))
    slot_ids = pair_of(jnp.arange(group_rows, dtype=jnp.int32))
    live_mask = pair_of(pad_mask)
    inverse_freq = jnp.asarray(rope_table(HEAD_SIZE), f32)
    angles = pair_of(positions).astype(f32)[:, None] * inverse_freq[None, :]
    cosine_lookup = jnp.cos(angles)
    sine_lookup = jnp.sin(angles)
    query_head_split = rotary_apply(
        qkv[:, :query_cols].reshape(group_rows, heads_query, HEAD_SIZE),
        cosine_lookup,
        sine_lookup,
        1.0,
    )
    query_head_split = query_head_split.astype(bf16).reshape(
        group_rows, heads_kv, group_size, HEAD_SIZE
    )
    key_head_split = rotary_apply(
        qkv[:, query_cols : query_cols + key_cols].reshape(group_rows, heads_kv, HEAD_SIZE),
        cosine_lookup,
        sine_lookup,
        1.0,
    ).astype(bf16)
    value_head_split = (
        qkv[:, query_cols + key_cols :].astype(bf16).reshape(group_rows, heads_kv, HEAD_SIZE)
    )
    segment = (slot_ids >= seq_lens[0]).astype(jnp.int32)
    allowed = (
        (segment[:, None] == segment[None, :])
        & (slot_ids[None, :] <= slot_ids[:, None])
        & ((live_mask[None, :] == 1) | (slot_ids[:, None] == slot_ids[None, :]))
    )
    scores = (
        jnp.einsum("qgmd,kgd->gmqk", query_head_split, key_head_split, preferred_element_type=f32)
        * score_scale
    )
    scores = jnp.where(allowed[None, None], scores, -1e30)
    row_peak = jnp.max(scores, axis=-1, keepdims=True)
    log_total = row_peak + jnp.log(jnp.sum(jnp.exp(scores - row_peak), axis=-1, keepdims=True))
    probs_low = jnp.exp(scores - log_total).astype(bf16)
    attended = jnp.einsum("gmqk,kgd->qgmd", probs_low, value_head_split, preferred_element_type=f32)
    attended = attended.reshape(group_rows, heads_query * HEAD_SIZE).astype(bf16)
    both_full = gather_hidden([after(part, attended) for part in both_got])
    down_full = gather_hidden(axes.exchange_z([after(part, both_full) for part in down_parts]))

    def split_sum(pieces):
        sent = jnp.concatenate([piece(slice(own_rows, None)) for piece in pieces], axis=1)
        got = axes.over_y(sent.astype(bf16))
        kept = jnp.concatenate([piece(slice(0, own_rows)) for piece in pieces], axis=1)
        return kept + got.astype(f32)

    branch = split_sum(
        [lambda rows, i=i: contract_cols(attended[rows], out_pieces[i]) for i in range(4)]
    )
    resid = inputs_wide + branch
    inverse_two = lax.rsqrt(jnp.mean(resid * resid, axis=1, keepdims=True) + eps)
    normed_two = (resid * inverse_two).astype(bf16)

    def gather_tokens(own):
        parts = axes.gather_z(own)
        return jnp.concatenate(parts + [axes.over_y(part) for part in parts], axis=0)

    normed_two_all = gather_tokens(normed_two)
    cotangent_all = gather_tokens(after(cotangent_low, normed_two_all))
    line_rows = n * own_rows
    gate_up = dot(normed_two_all, both_full)
    gate_proj, up_proj = gate_up[:, :hidden_cols], gate_up[:, hidden_cols:]
    sigmoid_gate = jax.nn.sigmoid(gate_proj)
    gate_active = gate_proj * sigmoid_gate
    hidden = (gate_active * up_proj).astype(bf16)
    hidden_grad = dot(cotangent_all, down_full)
    gate_grad = (
        hidden_grad * up_proj * sigmoid_gate * (1.0 + gate_proj * (1.0 - sigmoid_gate))
    ).astype(bf16)
    up_grad = (hidden_grad * gate_active).astype(bf16)
    both_grad = jnp.concatenate([gate_grad, up_grad], axis=1)

    def scatter_tokens(left, right):
        sent = contract_cols(left[line_rows:], right).astype(bf16)
        got = [
            axes.over_y(sent[s * own_rows : (s + 1) * own_rows]) for s in range(n)
        ]
        kept = contract_cols(left[:line_rows], right)
        total = axes.scatter_z(
            [
                kept[s * own_rows : (s + 1) * own_rows] + got[s].astype(f32)
                for s in range(n)
            ]
        )
        return total, got[0]

    normed_two_grad, _ = scatter_tokens(both_grad, both_full)
    branch_feed, feed_got = scatter_tokens(after(hidden, normed_two_grad), down_full)
    output = reorder((resid + branch_feed).astype(bf16), to_place)

    down_sums, _ = axes.reduce_rows(cotangent_all, hidden)
    both_sums, both_beside = axes.reduce_rows(normed_two_all, both_grad)
    down_got = axes.exchange_z(down_sums)
    both_got = axes.exchange_z(both_sums)
    grad_gate, grad_up, grad_down, gain_two_sum = finish_ffn(
        axes, both_got, down_got, scale_ffn, gate_weight, up_weight
    )

    resid_grad = cotangent_low.astype(f32) + norm_back(resid, inverse_two, normed_two_grad)
    resid_low_all = pair_rows(resid_grad.astype(bf16))
    attended_grad = sum(dot(columns(resid_low_all, i), out_pieces[i]) for i in range(4))
    out_sum = axes.scatter_z(
        axes.reduce_rows(resid_low_all, attended, both_sums[1])[0]
    )
    attended_heads = attended_grad.astype(bf16).reshape(
        group_rows, heads_kv, group_size, HEAD_SIZE
    )
    probs_full = jnp.exp(scores - log_total)
    prob_grad = jnp.einsum(
        "qgmd,kgd->gmqk", attended_heads, value_head_split, preferred_element_type=f32
    )
    row_delta = jnp.sum(prob_grad * probs_full, axis=-1, keepdims=True)
    score_grad = after((probs_full * (prob_grad - row_delta)).astype(bf16), both_beside, feed_got)
    value_grad = jnp.einsum("gmqk,qgmd->kgd", probs_low, attended_heads, preferred_element_type=f32)
    value_grad = value_grad.reshape(group_rows, key_cols).astype(bf16)
    query_grad = (
        jnp.einsum("gmqk,kgd->qgmd", score_grad, key_head_split, preferred_element_type=f32)
        * score_scale
    )
    query_grad = rotary_apply(
        query_grad.reshape(group_rows, heads_query, HEAD_SIZE), cosine_lookup, sine_lookup, -1.0
    )
    query_grad = query_grad.reshape(group_rows, query_cols).astype(bf16)
    key_grad = (
        jnp.einsum("gmqk,qgmd->kgd", score_grad, query_head_split, preferred_element_type=f32)
        * score_scale
    )
    key_grad = (
        rotary_apply(key_grad, cosine_lookup, sine_lookup, -1.0)
        .reshape(group_rows, key_cols)
        .astype(bf16)
    )
    qkv_grad = jnp.concatenate([query_grad, key_grad, value_grad], axis=1)
    normed_one_grad = split_sum(
        [lambda rows, i=i: contract_cols(qkv_grad[rows], qkv_pieces[i]) for i in range(4)]
    )
    qkv_sum = axes.scatter_z(axes.reduce_rows(normed_one_all, qkv_grad)[0])
    token_grad = reorder(
        resid_grad + norm_back(inputs_wide, inverse_one, normed_one_grad), to_place
    )
    gain_one_sum = jnp.sum(qkv_sum * own_qkv.astype(f32), axis=1)
    qkv_out = qkv_sum * scale_attn

    def share(vector):
        total = vector + axes.over_y(vector)
        return lax.dynamic_slice_in_dim(total, axes.y * (block // 2), block // 2)

    return (
        output,
        token_grad,
        share(gain_one_sum),
        qkv_out[:, :query_cols],
        qkv_out[:, query_cols : query_cols + key_cols],
        qkv_out[:, query_cols + key_cols :],
        out_sum.T,
        share(gain_two_sum[:, 0]),
        grad_gate,
        grad_up,
        grad_down,
    )


def solution(mesh):
    dp = mesh.shape["dp"]
    placed = (
        P(("dp", "tp"), None),
        P("dp"),
        P("dp", "tp"),
        P("dp", "tp"),
        P("dp", "tp"),
        P("tp", "dp"),
        P("dp"),
        P("dp", "tp"),
        P("dp", "tp"),
        P("tp", "dp"),
        P(("dp", "tp"), None),
        P("dp"),
        P("dp"),
        P("dp"),
    )

    def program(*arrays):
        return shards(dp, *arrays)

    return jax.shard_map(
        program,
        mesh=mesh,
        in_specs=placed,
        out_specs=(
            P(("dp", "tp"), None),
            P(("dp", "tp"), None),
            P(("dp", "tp")),
            P("dp", "tp"),
            P("dp", "tp"),
            P("dp", "tp"),
            P("tp", "dp"),
            P(("dp", "tp")),
            P("dp", "tp"),
            P("dp", "tp"),
            P("tp", "dp"),
        ),
        check_vma=False,
    )
```
